32 devices in a mesh: group: 8 (over z, y), peer: 4 (over x, core).
Axes of the slice: x: 2, y: 2, z: 4, core: 2. Of those that a mesh axis runs over, the one named last changes fastest.
Arguments:
- features: float32 [128, 64, 384], P('group', 'peer'), may hold values from -6 to 6
- image_of_row: int32 [8], replicated, may hold values from 0 to 3, never falling along the last dimension, each value on 1 to 4 neighbouring positions
- llm_peer: int32 [32, 1], P(('group', 'peer')), may hold values from 0 to 3, as said below
- token_grads: float32 [64, 64, 384], P(('group', 'peer')), may hold values from -6 to 6
- dw_weight: float32 [49, 384], replicated, may hold values from -0.875 to 0.875
- dw_bias: float32 [384], replicated, may hold values from -3 to 3
- ln_gain: float32 [384], replicated, may hold values from 0.1 to 1.9
- ln_bias: float32 [384], replicated, may hold values from -3 to 3
- w_in: bfloat16 [384, 1536], replicated, may hold values from -0.3125 to 0.3125
- b_in: float32 [1536], replicated, may hold values from -3 to 3
- w_out: bfloat16 [1536, 384], replicated, may hold values from -0.15625 to 0.15625
- b_out: float32 [384], replicated, may hold values from -3 to 3
- layer_scale: float32 [384], replicated, may hold values from 0.3 to 1
- comp_weight: bfloat16 [9, 384, 384], replicated, may hold values from -0.109375 to 0.109375
- comp_bias: float32 [384], replicated, may hold values from -3 to 3
Outputs:
- llm_tokens: float32 [64, 64, 384], P(('group', 'peer'))
- feature_grads: float32 [128, 64, 384], P('group', 'peer')
The draws below stay inside these ranges and needn't reach their ends.
Inputs may be any that keep to these rules, and one draw needn't show every extreme that they name: `llm_peer`: the 1 tiles of one device go to 1 different peers of its group; each peer receives at most 2 tiles of its tile row, and in tile row 0 some peer receives exactly 2. `image_of_row`: Non-decreasing along tile rows; each image spans 1 to 4 consecutive tile rows.
All inputs are finite; a program needn't handle non-finite values.
Results may differ from the reference program's by a relative error of at most 0.005.
Values sent between devices are 32-bit elements; how exact they have to be, the bound alone decides.
A program may use at most 64 MiB of HBM per device.

```python
import math
import jax
import jax.numpy as jnp
import numpy as np
from jax import lax

C = 384
HID = 1536
SIDE = 16
TPD = 1
CAP = 2
POOLED = 8
IMAGES = 4
N_GROUP = 8
N_PEER = 4


def draw_llm_peer(key, part):
    order_key = jax.random.fold_in(key, 11)
    law_key = jax.random.fold_in(key, 12)
    row_keys = jax.random.split(order_key, N_GROUP)
    orders = jax.vmap(lambda k: jax.random.permutation(k, N_PEER))(row_keys).astype(jnp.int32)
    position = jnp.argsort(orders, axis=1, stable=True).astype(jnp.int32)
    lawbit = jax.random.randint(law_key, (N_GROUP,), 0, 2).astype(jnp.int32)
    lawbit = lawbit.at[0].set(1)
    tile_num = jnp.arange(TPD, dtype=jnp.int32)
    half_count = N_PEER // 2
    skewed = (position[:, :, None] // 2 + tile_num[None, None, :]) % half_count
    even = (position[:, :, None] + tile_num[None, None, :]) % N_PEER
    chosen = jnp.where(lawbit[:, None, None] == 1, skewed, even)
    dest = jnp.take_along_axis(orders[:, None, :], chosen.reshape(N_GROUP, 1, N_PEER * TPD), axis=2)
    return dest.reshape(N_GROUP * N_PEER * TPD, 1).astype(jnp.int32)


def block_scale(stream_key, dims, cuts, least, top_value):
    factor_of, own = 1.0, jax.random.fold_in(stream_key, 6)
    for axis_at, shards_of in cuts:
        steps = jnp.exp(jax.random.uniform(jax.random.fold_in(own, axis_at), (shards_of,), jnp.float32, least / len(cuts), top_value / len(cuts)))
        factor_of = factor_of * jnp.repeat(steps, dims[axis_at] // shards_of).reshape([-1 if axis == axis_at else 1 for axis in range(len(dims))])
    return factor_of


def length_profile(amount, total, limit, lean):
    loads = [(1 << 20) // math.isqrt(rank ** lean) + 1 for rank in range(2, amount + 1)]
    rest, counts = total - limit - (amount - 1), [1] * (amount - 1)
    while rest > 0:
        movable = [i for i in range(amount - 1) if counts[i] < limit]
        mass, budget = sum([loads[i] for i in movable]), rest
        for i in movable:
            more = min(limit - counts[i], max(1, budget * loads[i] // mass), rest)
            counts[i] = counts[i] + more
            rest = rest - more
    return np.array([limit] + counts)


def ragged(own_key, count, total, reach, skew):
    if count == 2:
        one = jax.random.randint(own_key, (), max(1, total - reach), min(reach, total - 1) + 1)
        return jnp.stack([one, total - one])
    tallies = jnp.asarray(length_profile(count, total, reach, skew), jnp.int32)
    couples = (count - 1) // 2
    source_of, sink = tallies[1:1 + 2 * couples:2], tallies[2:2 + 2 * couples:2]
    margin = jnp.minimum(source_of - 1, reach - sink)
    moved = jax.random.randint(jax.random.fold_in(own_key, 1), (couples,), 0, 1 << 20) % (margin + 1)
    tallies = tallies.at[1:1 + 2 * couples:2].set(source_of - moved).at[2:2 + 2 * couples:2].set(sink + moved)
    return tallies[jax.random.permutation(jax.random.fold_in(own_key, 2), count)]


def normal_values(stream_key, shape, spread, limit, pieces=(), kind=jnp.bfloat16):
    level = block_scale(stream_key, shape, pieces, -0.22, 0.18) if pieces else 1.0
    array = jax.random.normal(stream_key, shape, jnp.float32) * spread * level
    return jnp.minimum(jnp.maximum(array, -limit), limit).astype(kind)


def setup_inputs(seed: int = 0) -> dict:
    arg_keys = jax.random.split(jax.random.key(seed), 16)
    return {
        "features": normal_values(arg_keys[0], (N_GROUP * SIDE, N_PEER * TPD * SIDE, C), 1.0, 6.0, ((0, 8), (1, 4)), jnp.float32),
        "image_of_row": jnp.searchsorted(jnp.cumsum(ragged(arg_keys[1], IMAGES, N_GROUP, 4, 1)), jnp.arange(N_GROUP), side="right").astype(jnp.int32),
        "llm_peer": draw_llm_peer(jax.random.fold_in(arg_keys[15], 71), 0),
        "token_grads": normal_values(arg_keys[3], (N_GROUP * N_PEER * CAP, POOLED * POOLED, C), 1.0, 6.0, ((0, 32),), jnp.float32),
        "dw_weight": normal_values(arg_keys[4], (49, C), 49 ** -0.5, 0.875, (), jnp.float32),
        "dw_bias": normal_values(arg_keys[5], (C,), 0.5, 3.0, (), jnp.float32),
        "ln_gain": jnp.clip(1.0 + 0.18 * jax.random.normal(arg_keys[6], (C,), jnp.float32), 0.1, 1.9),
        "ln_bias": normal_values(arg_keys[7], (C,), 0.5, 3.0, (), jnp.float32),
        "w_in": normal_values(arg_keys[8], (C, HID), C ** -0.5, 0.3125),
        "b_in": normal_values(arg_keys[9], (HID,), 0.5, 3.0, (), jnp.float32),
        "w_out": normal_values(arg_keys[10], (HID, C), HID ** -0.5, 0.15625),
        "b_out": normal_values(arg_keys[11], (C,), 0.5, 3.0, (), jnp.float32),
        "layer_scale": jnp.clip(jnp.exp(jax.random.uniform(arg_keys[12], (C,), jnp.float32, math.log(0.3), math.log(1.0))), 0.3, 1.0),
        "comp_weight": normal_values(arg_keys[13], (9, C, C), (9 * C) ** -0.5, 0.109375),
        "comp_bias": normal_values(arg_keys[14], (C,), 0.5, 3.0, (), jnp.float32),
    }


def encode(tile_data, params):
    dw_weight, dw_bias, ln_gain, ln_bias, w_in, b_in, w_out, b_out, layer_scale = params
    tile_side = tile_data.shape[1]
    channels = tile_data.shape[3]
    padded = jnp.pad(tile_data, ((0, 0), (3, 3), (3, 3), (0, 0)))
    spatial = jnp.zeros_like(tile_data) + dw_bias
    for offset in range(49):
        row_off = offset // 7
        col_off = offset % 7
        spatial = spatial + padded[:, row_off:row_off + tile_side, col_off:col_off + tile_side, :] * dw_weight[offset]
    average = lax.optimization_barrier(jnp.mean(spatial, axis=-1, keepdims=True))
    centered = spatial - average
    variance = lax.optimization_barrier(jnp.mean(centered * centered, axis=-1, keepdims=True))
    normed = centered * lax.rsqrt(variance + 1e-06) * ln_gain + ln_bias
    flattened = normed.reshape(-1, channels).astype(jnp.bfloat16)
    hidden = jax.nn.gelu(jnp.dot(flattened, w_in, preferred_element_type=jnp.float32) + b_in, approximate=False)
    branch = jnp.dot(hidden.astype(jnp.bfloat16), w_out, preferred_element_type=jnp.float32) + b_out
    return tile_data + layer_scale * branch.reshape(tile_data.shape)

def pool_tiles(tile_data):
    tile_count, tile_side, other_side, channels = tile_data.shape
    return tile_data.reshape(tile_count, tile_side // 2, 2, other_side // 2, 2, channels).mean(axis=(2, 4))

def spread_tiles(grad_data):
    return jnp.repeat(jnp.repeat(grad_data, 2, axis=1), 2, axis=2) * 0.25

def compress_conv(padded, kernel):
    out_rows = padded.shape[-3] - 2
    out_cols = padded.shape[-2] - 2
    leading = padded.shape[:-3]
    summed = jnp.zeros((1, kernel.shape[2]), jnp.float32)
    for offset in range(9):
        row_off = offset // 3
        col_off = offset % 3
        window = padded[..., row_off:row_off + out_rows, col_off:col_off + out_cols, :]
        window = window.reshape(-1, padded.shape[-1]).astype(jnp.bfloat16)
        summed = summed + jnp.dot(window, kernel[offset], preferred_element_type=jnp.float32)
    return summed.reshape(leading + (out_rows, out_cols, kernel.shape[2]))

def rim_pad(pool_grid, keep_up, keep_down):
    empty = jnp.zeros_like(pool_grid[:1, 0])
    above = jnp.concatenate([empty, pool_grid[:-1, -1]], axis=0) * keep_up[:, None, None]
    below = jnp.concatenate([pool_grid[1:, 0], empty], axis=0) * keep_down[:, None, None]
    stacked = jnp.concatenate([above[:, None], pool_grid, below[:, None]], axis=1)
    return jnp.pad(stacked, ((0, 0), (0, 0), (1, 1), (0, 0)))

def reference(features, image_of_row, llm_peer, token_grads, dw_weight, dw_bias, ln_gain, ln_bias, w_in, b_in, w_out, b_out, layer_scale, comp_weight, comp_bias):
    params = (dw_weight, dw_bias, ln_gain, ln_bias, w_in, b_in, w_out, b_out, layer_scale)
    groups = N_GROUP
    peer_count = N_PEER
    per_row = peer_count * TPD
    channels = features.shape[2]
    tile_groups = features.reshape(groups, SIDE, per_row, SIDE, channels).transpose(0, 2, 1, 3, 4)

    def run_block(tile_data):
        return encode(tile_data, params)
    encoded = lax.map(run_block, tile_groups)
    pooled = pool_tiles(encoded.reshape(-1, SIDE, SIDE, channels))
    pooled = pooled.reshape(groups, per_row, POOLED, POOLED, channels)
    pool_grid = pooled.transpose(0, 2, 1, 3, 4).reshape(groups, POOLED, per_row * POOLED, channels)
    same_image = (image_of_row[1:] == image_of_row[:-1]).astype(jnp.float32)
    zero_one = jnp.zeros((1,), jnp.float32)
    keep_up = jnp.concatenate([zero_one, same_image])
    keep_down = jnp.concatenate([same_image, zero_one])
    compressed = compress_conv(rim_pad(pool_grid, keep_up, keep_down), comp_weight) + comp_bias
    comp_tiles = compressed.reshape(groups, POOLED, peer_count, TPD, POOLED, channels)
    comp_tiles = comp_tiles.transpose(0, 2, 3, 1, 4, 5).reshape(groups, peer_count, TPD, POOLED * POOLED, channels)
    route_hot = (llm_peer.reshape(groups, peer_count, TPD)[..., None] == jnp.arange(peer_count, dtype=jnp.int32)).astype(jnp.float32)
    sends = lax.optimization_barrier(jnp.sum(route_hot, axis=2))
    before = jnp.cumsum(sends, axis=1) - sends
    slot_hot = (before[..., None] == jnp.arange(CAP, dtype=jnp.int32).astype(jnp.float32)).astype(jnp.float32)
    full_hot = route_hot[..., None] * slot_hot[:, :, None]
    llm_tokens = jnp.einsum('gptds,gptxc->gdsxc', full_hot, comp_tiles, precision=lax.Precision.HIGHEST)
    llm_tokens = llm_tokens.reshape(groups * peer_count * CAP, POOLED * POOLED, channels)
    incoming = token_grads.reshape(groups, peer_count, CAP, POOLED * POOLED, channels)
    grad_tiles = jnp.einsum('gptds,gdsxc->gptxc', full_hot, incoming, precision=lax.Precision.HIGHEST)
    grad_grid = grad_tiles.reshape(groups, peer_count, TPD, POOLED, POOLED, channels)
    grad_grid = grad_grid.transpose(0, 3, 1, 2, 4, 5).reshape(groups, POOLED, per_row * POOLED, channels)
    flipped = jnp.transpose(comp_weight[::-1], (0, 2, 1))
    grad_pooled = compress_conv(rim_pad(grad_grid, keep_up, keep_down), flipped)
    grad_pooled = grad_pooled.reshape(groups, POOLED, per_row, POOLED, channels).transpose(0, 2, 1, 3, 4)
    grad_encoded = spread_tiles(grad_pooled.reshape(-1, POOLED, POOLED, channels))
    grad_encoded = grad_encoded.reshape(groups, per_row, SIDE, SIDE, channels)

    def pull_back(pair):
        tile_data, grad_data = pair
        pullback = jax.vjp(run_block, tile_data)[1]
        return pullback(grad_data)[0]
    grad_input = lax.map(pull_back, (tile_groups, grad_encoded))
    feature_grads = grad_input.transpose(0, 2, 1, 3, 4).reshape(groups * SIDE, per_row * SIDE, channels)
    return (llm_tokens, feature_grads)
```

```python
import functools
import math

import jax
import jax.numpy as jnp
from jax import lax
from jax.experimental import pallas as pl
from jax.experimental.pallas import tpu as pltpu
from jax.sharding import PartitionSpec as P

MESH = pl.DeviceIdType.MESH
LANES = 128
PAD = 8
BLOCK = 256
ROWS = ((-1, -1), (-1, 0), (-1, 1), (0, -1), (0, 1), (1, -1), (1, 0), (1, 1))


def nt_dot(a, b):
    return lax.dot_general(a, b, (((1,), (1,)), ((), ())), preferred_element_type=jnp.float32)


def depthwise(src, weight, chunk, taps, side, flip):
    half = side // 2
    reach = taps // 2
    outs = []
    for parity in range(2):
        total = None
        for b in range(taps):
            rows = src[chunk, :, pl.ds(PAD - reach + parity + b, half, stride=2), :]
            for a in range(taps):
                k = (taps - 1 - a) * taps + taps - 1 - b if flip else a * taps + b
                term = rows[a : a + side] * weight[chunk, k : k + 1, :]
                total = term if total is None else total + term
        outs.append(total)
    return outs


def kernel(
    groups,
    peers,
    taps,
    image_hbm,
    owner_hbm,
    x_hbm,
    tg_hbm,
    dww_hbm,
    dwb_hbm,
    gain_hbm,
    lnb_hbm,
    win_hbm,
    bin_hbm,
    wout_hbm,
    bout_hbm,
    scale_hbm,
    cw_hbm,
    cb_hbm,
    tok_hbm,
    dx_hbm,
    xpad,
    gpad,
    dww,
    dwb,
    gain,
    lnb,
    bout,
    scale,
    cb,
    bin_,
    win,
    wout,
    cw,
    tg,
    sp,
    rstd,
    nb,
    dg,
    hb,
    dpb,
    table,
    sendg,
    recvg,
    tok,
    recvt,
    tokout,
    grid_g,
    grid_p,
    col_g,
    col_p,
    halo_g,
    halo_p,
    gq,
    obuf,
    image_ref,
    owner_ref,
    in_sems,
    out_sems,
    tab_send,
    tab_recv,
    g_send,
    g_recv,
    t_send,
    t_recv,
    hg_send,
    hg_recv,
    hp_send,
    hp_recv,
):
    g = lax.axis_index("group")
    me = lax.axis_index("peer")
    side = x_hbm.shape[0]
    channels = x_hbm.shape[2]
    half = side // 2
    cells = half * half
    chunks = channels // LANES
    reach = taps // 2
    hid = win.shape[1]
    slots = tg.shape[0]
    small = (dwb, gain, lnb, bout, scale, cb)

    def vector(ref, lane=slice(None)):
        return ref[lane].reshape(1, -1)

    halo_g[...] = jnp.zeros_like(halo_g)
    halo_p[...] = jnp.zeros_like(halo_p)
    barrier = pltpu.get_barrier_semaphore()

    def there(dr, dp):
        conds = []
        if dr < 0:
            conds.append(g > 0)
        if dr > 0:
            conds.append(g < groups - 1)
        if dp < 0:
            conds.append(me > 0)
        if dp > 0:
            conds.append(me < peers - 1)
        cond = conds[0]
        for other in conds[1:]:
            cond = jnp.logical_and(cond, other)
        return cond

    for k in range(1, peers):
        pl.semaphore_signal(
            barrier, inc=1, device_id={"group": g, "peer": lax.rem(me + k, peers)}, device_id_type=MESH
        )
    for dr, dp in ROWS:
        if dr != 0:

            @pl.when(there(dr, dp))
            def _():
                pl.semaphore_signal(
                    barrier, inc=1, device_id={"group": g + dr, "peer": me + dp}, device_id_type=MESH
                )

    copies = {}

    def fetch(name, src, dst):
        copy = pltpu.make_async_copy(src, dst, in_sems.at[len(copies)])
        copy.start()
        copies[name] = copy

    fetch("owner", owner_hbm, owner_ref)
    for c in range(chunks):
        lane = slice(c * LANES, (c + 1) * LANES)
        fetch(("w", c), dww_hbm.at[:, lane], dww.at[c])
        fetch(("x", c), x_hbm.at[:, :, lane], xpad.at[c, reach : reach + side, PAD : PAD + side, :])
    for i, src in enumerate((dwb_hbm, gain_hbm, lnb_hbm, bout_hbm, scale_hbm, cb_hbm)):
        fetch(("s", i), src, small[i])
    fetch("tg", tg_hbm, tg)
    fetch("image", image_hbm, image_ref)
    fetch("bin", bin_hbm, bin_)
    fetch("win", win_hbm, win)
    fetch("wout", wout_hbm, wout)
    fetch("cw", cw_hbm, cw)

    def clear(buf):
        width = buf.shape[2]
        for c in range(chunks):
            buf[c, :reach] = jnp.zeros((reach, width, LANES), jnp.float32)
            buf[c, reach + side :] = jnp.zeros((reach, width, LANES), jnp.float32)
            buf[c, reach : reach + side, :PAD] = jnp.zeros((side, PAD, LANES), jnp.float32)
            buf[c, reach : reach + side, PAD + side :] = jnp.zeros((side, PAD, LANES), jnp.float32)

    clear(xpad)
    clear(gpad)
    copies["owner"].wait()
    own = owner_ref[0, 0]
    table[me] = jnp.full((8, LANES), own, jnp.int32)

    def forward_conv(c):
        outs = depthwise(xpad, dww, c, taps, side, False)
        bias = vector(small[0], slice(c * LANES, (c + 1) * LANES))
        for parity in range(2):
            part = (outs[parity] + bias).reshape(half, 2, half, LANES)
            for row in range(2):
                sp[c, row * 2 + parity] = part[:, row].reshape(cells, LANES)

    copies[("s", 0)].wait()
    for c in range(chunks):
        copies[("w", c)].wait()
        copies[("x", c)].wait()
    forward_conv(0)

    across = 1 + (me > 0).astype(jnp.int32) + (me < peers - 1).astype(jnp.int32)
    along = (g > 0).astype(jnp.int32) + (g < groups - 1).astype(jnp.int32)
    pl.semaphore_wait(barrier, peers - 1 + across * along)

    def all_peers(src_of, dst_of, send, recv):
        moves = []
        for k in range(1, peers):
            moves.append(
                pltpu.make_async_remote_copy(
                    src_ref=src_of(k),
                    dst_ref=dst_of(k),
                    send_sem=send.at[k - 1],
                    recv_sem=recv.at[k - 1],
                    device_id={"group": g, "peer": lax.rem(me + k, peers)},
                    device_id_type=MESH,
                )
            )
        return moves

    table_moves = all_peers(lambda k: table.at[me], lambda k: table.at[me], tab_send, tab_recv)
    for move in table_moves:
        move.start()
    forward_conv(1)
    for move in table_moves:
        move.wait()
    copies["tg"].wait()

    def place_of(who):
        mine = table[who] == me
        before = jnp.zeros((8, LANES), jnp.int32)
        for p in range(peers):
            earlier = (p < who).astype(jnp.int32)
            before = before + jnp.where(table[p] == me, earlier, 0)
        return mine, before

    def wide(mask):
        return jnp.concatenate([mask.astype(jnp.float32)] * chunks, axis=1)

    def block_for(who):
        mine, before = place_of(who)
        total = None
        for s in range(slots):
            part = tg[s] * wide(jnp.logical_and(mine, before == s))
            total = part if total is None else total + part
        return total

    grad_moves = all_peers(lambda k: sendg.at[k - 1], lambda k: recvg.at[k - 1], g_send, g_recv)
    for k in range(1, peers):
        sendg[k - 1] = block_for(lax.rem(me + k, peers))
        grad_moves[k - 1].start()
    grid_g[1 : half + 1, PAD : PAD + half, :] = block_for(me)
    for c in range(2, chunks):
        forward_conv(c)

    for i in range(1, 6):
        copies[("s", i)].wait()
    for q in range(4):
        parts = [sp[c, q] for c in range(chunks)]
        mean = jnp.sum(functools.reduce(jnp.add, parts), axis=1, keepdims=True) / channels
        parts = [part - mean for part in parts]
        square = functools.reduce(jnp.add, [part * part for part in parts])
        inv = lax.rsqrt(jnp.sum(square, axis=1, keepdims=True) / channels + 1e-06)
        rstd[q] = jnp.broadcast_to(inv, (cells, LANES))
        for c in range(chunks):
            lane = slice(c * LANES, (c + 1) * LANES)
            hat = parts[c] * inv
            sp[c, q] = hat
            nb[q * cells : (q + 1) * cells, lane] = (
                hat * vector(small[1], lane) + vector(small[2], lane)
            ).astype(jnp.bfloat16)

    def halo_moves(grid, col, halo, send, recv):
        moves = []
        for i, (dr, dp) in enumerate(ROWS):
            if dr == 0:
                src = col.at[0 if dp < 0 else 1]
            else:
                src = grid.at[1 if dr < 0 else half, PAD : PAD + half, :]
            back = len(ROWS) - 1 - i
            moves.append(
                pltpu.make_async_remote_copy(
                    src_ref=src,
                    dst_ref=halo.at[back],
                    send_sem=send.at[i],
                    recv_sem=recv.at[back],
                    device_id={"group": g + dr, "peer": me + dp},
                    device_id_type=MESH,
                )
            )
        return moves

    def halo_start(grid, col, moves):
        col[0] = grid[1 : half + 1, PAD, :]
        col[1] = grid[1 : half + 1, PAD + half - 1, :]
        for (dr, dp), move in zip(ROWS, moves):

            @pl.when(there(dr, dp))
            def _():
                move.start()

    def halo_finish(grid, halo, moves, send, recv):
        for i, (dr, dp) in enumerate(ROWS):

            @pl.when(there(dr, dp))
            def _():
                moves[i].wait_send()
                pltpu.make_async_remote_copy(
                    src_ref=halo.at[i],
                    dst_ref=halo.at[i],
                    send_sem=send.at[i],
                    recv_sem=recv.at[i],
                    device_id={"group": g + dr, "peer": me + dp},
                    device_id_type=MESH,
                ).wait_recv()

        image = image_ref[g]
        keep = {
            -1: (image_ref[jnp.maximum(g - 1, 0)] == image).astype(jnp.float32) * (g > 0).astype(jnp.float32),
            0: 1.0,
            1: (image_ref[jnp.minimum(g + 1, groups - 1)] == image).astype(jnp.float32)
            * (g < groups - 1).astype(jnp.float32),
        }
        edge = {-1: (me > 0).astype(jnp.float32), 0: 1.0, 1: (me < peers - 1).astype(jnp.float32)}
        for i, (dr, dp) in enumerate(ROWS):
            row = {-1: 0, 1: half + 1}.get(dr)
            factor = keep[dr] * edge[dp]
            if dr == 0:
                grid[1 : half + 1, PAD - 1 if dp < 0 else PAD + half, :] = halo[i] * factor
            elif dp == 0:
                grid[row, PAD : PAD + half, :] = halo[i] * factor
            elif dp < 0:
                grid[row, PAD - 1 : PAD, :] = halo[i, half - 1 : half, :] * factor
            else:
                grid[row, PAD + half : PAD + half + 1, :] = halo[i, 0:1, :] * factor

    def window(grid, a, b):
        part = grid[a : a + half, PAD - 1 + b : PAD - 1 + b + half, :]
        return part.reshape(cells, channels).astype(jnp.bfloat16)

    g_moves = halo_moves(grid_g, col_g, halo_g, hg_send, hg_recv)
    p_moves = halo_moves(grid_p, col_p, halo_p, hp_send, hp_recv)

    def gather_grads():
        total = grid_g[1 : half + 1, PAD : PAD + half, :]
        for k in range(1, peers):
            grad_moves[k - 1].wait()
            total = total + recvg[k - 1]
        grid_g[1 : half + 1, PAD : PAD + half, :] = total
        halo_start(grid_g, col_g, g_moves)

    copies["bin"].wait()
    copies["image"].wait()
    copies["win"].wait()
    for n in range(hid // BLOCK):
        lane = slice(n * BLOCK, (n + 1) * BLOCK)
        pre_all = jnp.dot(nb[...], win[:, lane], preferred_element_type=jnp.float32)
        bias = vector(bin_, lane)
        pooled = None
        for q in range(4):
            pre = pre_all[q * cells : (q + 1) * cells] + bias
            cdf = 0.5 + 0.5 * lax.erf(pre * math.sqrt(0.5))
            pdf = jnp.exp(pre * pre * -0.5) * (1.0 / math.sqrt(2.0 * math.pi))
            dg[q * cells : (q + 1) * cells, lane] = cdf + pre * pdf
            value = pre * cdf
            pooled = value if pooled is None else pooled + value
        hb[:, lane] = (pooled * 0.25).astype(jnp.bfloat16)
        if n == hid // BLOCK - 2:
            gather_grads()
    copies["wout"].wait()
    branch = jnp.dot(hb[...], wout[...], preferred_element_type=jnp.float32)
    for c in range(chunks):
        lane = slice(c * LANES, (c + 1) * LANES)
        total = None
        for row in range(2):
            for parity in range(2):
                part = xpad[c, reach : reach + side, pl.ds(PAD + parity, half, stride=2), :]
                part = part.reshape(half, 2, half, LANES)[:, row]
                total = part if total is None else total + part
        mixed = vector(small[4], lane) * (branch[:, lane] + vector(small[3], lane))
        grid_p[1 : half + 1, PAD : PAD + half, lane] = total * 0.25 + mixed.reshape(half, half, LANES)
    halo_start(grid_p, col_p, p_moves)

    copies["cw"].wait()
    halo_finish(grid_g, halo_g, g_moves, hg_send, hg_recv)
    grads = None
    for a in range(3):
        for b in range(3):
            part = nt_dot(window(grid_g, a, b), cw[(2 - a) * 3 + 2 - b])
            grads = part if grads is None else grads + part
    grads = grads * 0.25
    for c in range(chunks):
        lane = slice(c * LANES, (c + 1) * LANES)
        gq[c] = grads[:, lane].reshape(half, half, LANES)
    scaled = (grads * vector(scale)).astype(jnp.bfloat16)

    halo_finish(grid_p, halo_p, p_moves, hp_send, hp_recv)
    comp = None
    for a in range(3):
        for b in range(3):
            part = jnp.dot(window(grid_p, a, b), cw[a * 3 + b], preferred_element_type=jnp.float32)
            comp = part if comp is None else comp + part
    tok[...] = (comp + vector(cb)).reshape(half, half, channels)
    tok_moves = all_peers(lambda k: tok, lambda k: recvt.at[k - 1], t_send, t_recv)
    for move in tok_moves:
        move.start()

    for n in range(hid // BLOCK):
        lane = slice(n * BLOCK, (n + 1) * BLOCK)
        dh = nt_dot(scaled, wout[lane, :])
        for q in range(4):
            rows = slice(q * cells, (q + 1) * cells)
            dpb[rows, lane] = (dh * dg[rows, lane]).astype(jnp.bfloat16)
    for q in range(4):
        dn = nt_dot(dpb[q * cells : (q + 1) * cells, :], win[...]) * vector(gain)
        parts = [dn[:, c * LANES : (c + 1) * LANES] for c in range(chunks)]
        first = jnp.sum(functools.reduce(jnp.add, parts), axis=1, keepdims=True) / channels
        cross = functools.reduce(jnp.add, [parts[c] * sp[c, q] for c in range(chunks)])
        second = jnp.sum(cross, axis=1, keepdims=True) / channels
        for c in range(chunks):
            back = rstd[q] * (parts[c] - first - sp[c, q] * second)
            back = back.reshape(half, half, LANES)
            for i in range(half):
                gpad[c, reach + 2 * i + q // 2, pl.ds(PAD + q % 2, half, stride=2), :] = back[i]

    out_copies = []
    for c in range(chunks):
        outs = depthwise(gpad, dww, c, taps, side, True)
        direct = jnp.broadcast_to(gq[c][:, None], (half, 2, half, LANES)).reshape(side, half, LANES)
        for parity in range(2):
            value = outs[parity] + direct
            for i in range(side):
                obuf[c, i, pl.ds(parity, half, stride=2), :] = value[i]
        copy = pltpu.make_async_copy(
            obuf.at[c], dx_hbm.at[:, :, c * LANES : (c + 1) * LANES], out_sems.at[c]
        )
        copy.start()
        out_copies.append(copy)

    for move in tok_moves:
        move.wait()
    mine, before = place_of(me)
    outs = [tok[...] * wide(jnp.logical_and(mine, before == s)) for s in range(slots)]
    for k in range(1, peers):
        mine, before = place_of(lax.rem(me + peers - k, peers))
        for s in range(slots):
            outs[s] = outs[s] + recvt[k - 1] * wide(jnp.logical_and(mine, before == s))
    for s in range(slots):
        tokout[s] = outs[s]
    copy = pltpu.make_async_copy(tokout, tok_hbm, out_sems.at[chunks])
    copy.start()
    copy.wait()
    for copy in out_copies:
        copy.wait()


def solution(mesh):
    groups, peers = mesh.shape["group"], mesh.shape["peer"]

    def on_device(
        features, image_of_row, llm_peer, token_grads, dw_weight, dw_bias, ln_gain, ln_bias,
        w_in, b_in, w_out, b_out, layer_scale, comp_weight, comp_bias,
    ):
        side, width, channels = features.shape
        slots = token_grads.shape[0]
        hid = w_in.shape[1]
        taps = math.isqrt(dw_weight.shape[0])
        half = side // 2
        cells = half * half
        chunks = channels // LANES
        assert width == side and llm_peer.shape == (1, 1)
        f32, bf16 = jnp.float32, jnp.bfloat16
        padded = (chunks, side + 2 * (taps // 2), side + 2 * PAD, LANES)
        grid = (half + 2, half + 2 * PAD, channels)
        block = (half, half, channels)
        dma = pltpu.SemaphoreType.DMA
        hbm = pl.BlockSpec(memory_space=pl.ANY)
        tokens, grads = pl.pallas_call(
            functools.partial(kernel, groups, peers, taps),
            out_shape=(
                jax.ShapeDtypeStruct((slots,) + block, f32),
                jax.ShapeDtypeStruct(features.shape, f32),
            ),
            in_specs=[hbm] * 15,
            out_specs=(hbm, hbm),
            scratch_shapes=[
                pltpu.VMEM(padded, f32),
                pltpu.VMEM(padded, f32),
                pltpu.VMEM((chunks, taps * taps, LANES), f32),
                *[pltpu.VMEM((channels,), f32)] * 6,
                pltpu.VMEM((hid,), f32),
                pltpu.VMEM(w_in.shape, bf16),
                pltpu.VMEM(w_out.shape, bf16),
                pltpu.VMEM(comp_weight.shape, bf16),
                pltpu.VMEM((slots,) + block, f32),
                pltpu.VMEM((chunks, 4, cells, LANES), f32),
                pltpu.VMEM((4, cells, LANES), f32),
                pltpu.VMEM((4 * cells, channels), bf16),
                pltpu.VMEM((4 * cells, hid), f32),
                pltpu.VMEM((cells, hid), bf16),
                pltpu.VMEM((4 * cells, hid), bf16),
                pltpu.VMEM((peers, 8, LANES), jnp.int32),
                pltpu.VMEM((peers - 1,) + block, f32),
                pltpu.VMEM((peers - 1,) + block, f32),
                pltpu.VMEM(block, f32),
                pltpu.VMEM((peers - 1,) + block, f32),
                pltpu.VMEM((slots,) + block, f32),
                pltpu.VMEM(grid, f32),
                pltpu.VMEM(grid, f32),
                pltpu.VMEM((2, half, channels), f32),
                pltpu.VMEM((2, half, channels), f32),
                pltpu.VMEM((8, half, channels), f32),
                pltpu.VMEM((8, half, channels), f32),
                pltpu.VMEM((chunks, half, half, LANES), f32),
                pltpu.VMEM((chunks, side, side, LANES), f32),
                pltpu.SMEM(image_of_row.shape, jnp.int32),
                pltpu.SMEM((1, 1), jnp.int32),
                dma((2 * chunks + 13,)),
                dma((chunks + 1,)),
                dma((peers - 1,)),
                dma((peers - 1,)),
                dma((peers - 1,)),
                dma((peers - 1,)),
                dma((peers - 1,)),
                dma((peers - 1,)),
                dma((8,)),
                dma((8,)),
                dma((8,)),
                dma((8,)),
            ],
            compiler_params=pltpu.CompilerParams(collective_id=0, has_side_effects=True),
        )(
            image_of_row,
            llm_peer,
            features,
            token_grads.reshape((slots,) + block),
            dw_weight,
            dw_bias,
            ln_gain,
            ln_bias,
            w_in,
            b_in,
            w_out,
            b_out,
            layer_scale,
            comp_weight,
            comp_bias,
        )
        return tokens.reshape(slots, cells, channels), grads

    placed = [P()] * 15
    placed[0] = P("group", "peer", None)
    placed[2] = P(("group", "peer"), None)
    placed[3] = P(("group", "peer"), None, None)
    return jax.shard_map(
        on_device,
        mesh=mesh,
        in_specs=tuple(placed),
        out_specs=(P(("group", "peer"), None, None), P("group", "peer", None)),
        check_vma=False,
    )
```

```python
import functools
import math

import jax
import jax.numpy as jnp
from jax import lax
from jax.experimental import pallas as pl
from jax.experimental.pallas import tpu as pltpu
from jax.sharding import PartitionSpec as P

MESH = pl.DeviceIdType.MESH
LANES = 128
PAD = 8
BLOCK = 256
ROWS = ((-1, -1), (-1, 0), (-1, 1), (0, -1), (0, 1), (1, -1), (1, 0), (1, 1))


def nt_dot(a, b):
    return lax.dot_general(a, b, (((1,), (1,)), ((), ())), preferred_element_type=jnp.float32)


def depthwise(src, weight, chunk, taps, side, flip):
    half = side // 2
    reach = taps // 2
    outs = []
    for parity in range(2):
        total = None
        for b in range(taps):
            rows = src[chunk, :, pl.ds(PAD - reach + parity + b, half, stride=2), :]
            for a in range(taps):
                k = (taps - 1 - a) * taps + taps - 1 - b if flip else a * taps + b
                term = rows[a : a + side] * weight[chunk, k : k + 1, :]
                total = term if total is None else total + term
        outs.append(total)
    return outs


def kernel(
    groups,
    peers,
    taps,
    image_hbm,
    owner_hbm,
    x_hbm,
    tg_hbm,
    dww_hbm,
    dwb_hbm,
    gain_hbm,
    lnb_hbm,
    win_hbm,
    bin_hbm,
    wout_hbm,
    bout_hbm,
    scale_hbm,
    cw_hbm,
    cb_hbm,
    gpad,
    dww,
    gq,
    tokout,
    xpad,
    dwb,
    gain,
    lnb,
    bout,
    scale,
    cb,
    bin_,
    win,
    wout,
    cw,
    tg,
    sp,
    rstd,
    nb,
    dg,
    hb,
    dpb,
    table,
    sendg,
    recvg,
    sendf,
    recvf,
    tok,
    recvt,
    recvr,
    grid_g,
    grid_p,
    col_g,
    col_p,
    halo_g,
    halo_p,
    image_ref,
    owner_ref,
    in_sems,
    tab_send,
    tab_recv,
    near_send,
    near_recv,
    g_send,
    g_recv,
    t_send,
    t_recv,
    r_send,
    r_recv,
    hg_send,
    hg_recv,
    hp_send,
    hp_recv,
):
    g = lax.axis_index("group")
    me = lax.axis_index("peer")
    side = x_hbm.shape[0]
    channels = x_hbm.shape[2]
    half = side // 2
    cells = half * half
    chunks = channels // LANES
    reach = taps // 2
    hid = win.shape[1]
    slots = tg.shape[0]
    small = (dwb, gain, lnb, bout, scale, cb)

    def vector(ref, lane=slice(None)):
        return ref[lane].reshape(1, -1)

    halo_g[...] = jnp.zeros_like(halo_g)
    halo_p[...] = jnp.zeros_like(halo_p)
    barrier = pltpu.get_barrier_semaphore()

    def there(dr, dp):
        conds = []
        if dr < 0:
            conds.append(g > 0)
        if dr > 0:
            conds.append(g < groups - 1)
        if dp < 0:
            conds.append(me > 0)
        if dp > 0:
            conds.append(me < peers - 1)
        cond = conds[0]
        for other in conds[1:]:
            cond = jnp.logical_and(cond, other)
        return cond

    for k in range(1, peers):
        pl.semaphore_signal(
            barrier, inc=1, device_id={"group": g, "peer": lax.rem(me + k, peers)}, device_id_type=MESH
        )
    for dr, dp in ROWS:
        if dr != 0:

            @pl.when(there(dr, dp))
            def _():
                pl.semaphore_signal(
                    barrier, inc=1, device_id={"group": g + dr, "peer": me + dp}, device_id_type=MESH
                )

    copies = {}

    def fetch(name, src, dst):
        copy = pltpu.make_async_copy(src, dst, in_sems.at[len(copies)])
        copy.start()
        copies[name] = copy

    fetch("owner", owner_hbm, owner_ref)
    for c in range(chunks):
        lane = slice(c * LANES, (c + 1) * LANES)
        fetch(("w", c), dww_hbm.at[:, lane], dww.at[c])
        fetch(("x", c), x_hbm.at[:, :, lane], xpad.at[c, reach : reach + side, PAD : PAD + side, :])
    for i, src in enumerate((dwb_hbm, gain_hbm, lnb_hbm, bout_hbm, scale_hbm, cb_hbm)):
        fetch(("s", i), src, small[i])
    fetch("tg", tg_hbm, tg)
    fetch("image", image_hbm, image_ref)
    fetch("bin", bin_hbm, bin_)
    fetch("win", win_hbm, win)
    fetch("wout", wout_hbm, wout)
    fetch("cw", cw_hbm, cw)

    def clear(buf):
        width = buf.shape[2]
        for c in range(chunks):
            buf[c, :reach] = jnp.zeros((reach, width, LANES), jnp.float32)
            buf[c, reach + side :] = jnp.zeros((reach, width, LANES), jnp.float32)
            buf[c, reach : reach + side, :PAD] = jnp.zeros((side, PAD, LANES), jnp.float32)
            buf[c, reach : reach + side, PAD + side :] = jnp.zeros((side, PAD, LANES), jnp.float32)

    clear(xpad)
    clear(gpad)
    copies["owner"].wait()
    own = owner_ref[0, 0]
    table[me] = jnp.full((8, LANES), own, jnp.int32)

    def forward_conv(c):
        outs = depthwise(xpad, dww, c, taps, side, False)
        bias = vector(small[0], slice(c * LANES, (c + 1) * LANES))
        for parity in range(2):
            part = (outs[parity] + bias).reshape(half, 2, half, LANES)
            for row in range(2):
                sp[c, row * 2 + parity] = part[:, row].reshape(cells, LANES)

    across = 1 + (me > 0).astype(jnp.int32) + (me < peers - 1).astype(jnp.int32)
    along = (g > 0).astype(jnp.int32) + (g < groups - 1).astype(jnp.int32)
    pl.semaphore_wait(barrier, peers - 1 + across * along)

    table_moves = []
    for k in range(1, peers):
        table_moves.append(
            pltpu.make_async_remote_copy(
                src_ref=table.at[me],
                dst_ref=table.at[me],
                send_sem=tab_send.at[k - 1],
                recv_sem=tab_recv.at[k - 1],
                device_id={"group": g, "peer": lax.rem(me + k, peers)},
                device_id_type=MESH,
            )
        )
        table_moves[-1].start()
    copies[("s", 0)].wait()
    for c in range(chunks):
        copies[("w", c)].wait()
        copies[("x", c)].wait()
        forward_conv(c)
    for move in table_moves:
        move.wait()
    copies["tg"].wait()

    def place_of(who):
        mine = table[who] == me
        before = jnp.zeros((8, LANES), jnp.int32)
        for p in range(peers):
            earlier = (p < who).astype(jnp.int32)
            before = before + jnp.where(table[p] == me, earlier, 0)
        return mine, before

    def wide(mask):
        return jnp.concatenate([mask.astype(jnp.float32)] * chunks, axis=1)

    def block_for(who):
        mine, before = place_of(who)
        total = None
        for s in range(slots):
            part = tg[s] * wide(jnp.logical_and(mine, before == s))
            total = part if total is None else total + part
        return total

    pairs = peers // 2
    core = lax.rem(me, 2)
    partner = me + 1 - 2 * core

    def seat(k, which):
        return lax.rem(lax.div(me, 2) + k, pairs) * 2 + which

    def to(src, dst, send, recv, where):
        return pltpu.make_async_remote_copy(
            src_ref=src,
            dst_ref=dst,
            send_sem=send,
            recv_sem=recv,
            device_id={"group": g, "peer": where},
            device_id_type=MESH,
        )

    for k in range(pairs):
        sendg[k] = block_for(seat(k, 1 - core))
    near_move = to(sendg, recvg, near_send, near_recv, partner)
    near_move.start()
    grid_g[1 : half + 1, PAD : PAD + half, :] = block_for(me)
    far_moves = [
        to(sendf.at[k - 1], recvf.at[k - 1], g_send.at[k - 1], g_recv.at[k - 1], seat(k, core))
        for k in range(1, pairs)
    ]

    def pass_on():
        near_move.wait()
        for k in range(1, pairs):
            sendf[k - 1] = block_for(seat(k, core)) + recvg[k]
            far_moves[k - 1].start()

    for i in range(1, 6):
        copies[("s", i)].wait()
    for q in range(4):
        parts = [sp[c, q] for c in range(chunks)]
        mean = jnp.sum(functools.reduce(jnp.add, parts), axis=1, keepdims=True) / channels
        parts = [part - mean for part in parts]
        square = functools.reduce(jnp.add, [part * part for part in parts])
        inv = lax.rsqrt(jnp.sum(square, axis=1, keepdims=True) / channels + 1e-06)
        rstd[q] = jnp.broadcast_to(inv, (cells, LANES))
        for c in range(chunks):
            lane = slice(c * LANES, (c + 1) * LANES)
            hat = parts[c] * inv
            sp[c, q] = hat
            nb[q * cells : (q + 1) * cells, lane] = (
                hat * vector(small[1], lane) + vector(small[2], lane)
            ).astype(jnp.bfloat16)

    def halo_moves(grid, col, halo, send, recv):
        moves = []
        for i, (dr, dp) in enumerate(ROWS):
            if dr == 0:
                src = col.at[0 if dp < 0 else 1]
            else:
                src = grid.at[1 if dr < 0 else half, PAD : PAD + half, :]
            back = len(ROWS) - 1 - i
            moves.append(
                pltpu.make_async_remote_copy(
                    src_ref=src,
                    dst_ref=halo.at[back],
                    send_sem=send.at[i],
                    recv_sem=recv.at[back],
                    device_id={"group": g + dr, "peer": me + dp},
                    device_id_type=MESH,
                )
            )
        return moves

    def halo_start(grid, col, moves):
        col[0] = grid[1 : half + 1, PAD, :]
        col[1] = grid[1 : half + 1, PAD + half - 1, :]
        for (dr, dp), move in zip(ROWS, moves):

            @pl.when(there(dr, dp))
            def _():
                move.start()

    def halo_finish(grid, halo, moves, send, recv):
        for i, (dr, dp) in enumerate(ROWS):

            @pl.when(there(dr, dp))
            def _():
                moves[i].wait_send()
                pltpu.make_async_remote_copy(
                    src_ref=halo.at[i],
                    dst_ref=halo.at[i],
                    send_sem=send.at[i],
                    recv_sem=recv.at[i],
                    device_id={"group": g + dr, "peer": me + dp},
                    device_id_type=MESH,
                ).wait_recv()

        image = image_ref[g]
        keep = {
            -1: (image_ref[jnp.maximum(g - 1, 0)] == image).astype(jnp.float32) * (g > 0).astype(jnp.float32),
            0: 1.0,
            1: (image_ref[jnp.minimum(g + 1, groups - 1)] == image).astype(jnp.float32)
            * (g < groups - 1).astype(jnp.float32),
        }
        edge = {-1: (me > 0).astype(jnp.float32), 0: 1.0, 1: (me < peers - 1).astype(jnp.float32)}
        for i, (dr, dp) in enumerate(ROWS):
            row = {-1: 0, 1: half + 1}.get(dr)
            factor = keep[dr] * edge[dp]
            if dr == 0:
                grid[1 : half + 1, PAD - 1 if dp < 0 else PAD + half, :] = halo[i] * factor
            elif dp == 0:
                grid[row, PAD : PAD + half, :] = halo[i] * factor
            elif dp < 0:
                grid[row, PAD - 1 : PAD, :] = halo[i, half - 1 : half, :] * factor
            else:
                grid[row, PAD + half : PAD + half + 1, :] = halo[i, 0:1, :] * factor

    def window(grid, a, b):
        part = grid[a : a + half, PAD - 1 + b : PAD - 1 + b + half, :]
        return part.reshape(cells, channels).astype(jnp.bfloat16)

    g_moves = halo_moves(grid_g, col_g, halo_g, hg_send, hg_recv)
    p_moves = halo_moves(grid_p, col_p, halo_p, hp_send, hp_recv)

    def gather_grads():
        total = grid_g[1 : half + 1, PAD : PAD + half, :] + recvg[0]
        for k in range(1, pairs):
            far_moves[k - 1].wait()
            total = total + recvf[k - 1]
        grid_g[1 : half + 1, PAD : PAD + half, :] = total
        halo_start(grid_g, col_g, g_moves)

    copies["bin"].wait()
    copies["image"].wait()
    copies["win"].wait()
    for n in range(hid // BLOCK):
        lane = slice(n * BLOCK, (n + 1) * BLOCK)
        pre_all = jnp.dot(nb[...], win[:, lane], preferred_element_type=jnp.float32)
        bias = vector(bin_, lane)
        pooled = None
        for q in range(4):
            pre = pre_all[q * cells : (q + 1) * cells] + bias
            cdf = 0.5 + 0.5 * lax.erf(pre * math.sqrt(0.5))
            pdf = jnp.exp(pre * pre * -0.5) * (1.0 / math.sqrt(2.0 * math.pi))
            dg[q * cells : (q + 1) * cells, lane] = cdf + pre * pdf
            value = pre * cdf
            pooled = value if pooled is None else pooled + value
        hb[:, lane] = (pooled * 0.25).astype(jnp.bfloat16)
        if n == hid // BLOCK - 2:
            pass_on()
    copies["wout"].wait()
    branch = jnp.dot(hb[...], wout[...], preferred_element_type=jnp.float32)
    for c in range(chunks):
        lane = slice(c * LANES, (c + 1) * LANES)
        total = None
        for row in range(2):
            for parity in range(2):
                part = xpad[c, reach : reach + side, pl.ds(PAD + parity, half, stride=2), :]
                part = part.reshape(half, 2, half, LANES)[:, row]
                total = part if total is None else total + part
        mixed = vector(small[4], lane) * (branch[:, lane] + vector(small[3], lane))
        grid_p[1 : half + 1, PAD : PAD + half, lane] = total * 0.25 + mixed.reshape(half, half, LANES)
    halo_start(grid_p, col_p, p_moves)

    copies["cw"].wait()
    halo_finish(grid_p, halo_p, p_moves, hp_send, hp_recv)
    comp = None
    for a in range(3):
        for b in range(3):
            part = jnp.dot(window(grid_p, a, b), cw[a * 3 + b], preferred_element_type=jnp.float32)
            comp = part if comp is None else comp + part
    tok[...] = (comp + vector(cb)).reshape(half, half, channels)
    tok_moves = [to(tok, recvt.at[0], t_send.at[0], t_recv.at[0], partner)]
    for k in range(1, pairs):
        tok_moves.append(to(tok, recvt.at[k], t_send.at[k], t_recv.at[k], seat(k, core)))
    for move in reversed(tok_moves):
        move.start()
    gather_grads()

    halo_finish(grid_g, halo_g, g_moves, hg_send, hg_recv)
    grads = None
    for a in range(3):
        for b in range(3):
            part = nt_dot(window(grid_g, a, b), cw[(2 - a) * 3 + 2 - b])
            grads = part if grads is None else grads + part
    grads = grads * 0.25
    for c in range(chunks):
        lane = slice(c * LANES, (c + 1) * LANES)
        gq[c] = grads[:, lane].reshape(half, half, LANES)
    scaled = (grads * vector(scale)).astype(jnp.bfloat16)

    relays = []

    def relay():
        for k in range(1, pairs):
            tok_moves[k].wait()
            relays.append(to(recvt.at[k], recvr.at[k - 1], r_send.at[k - 1], r_recv.at[k - 1], partner))
            relays[-1].start()

    for n in range(hid // BLOCK):
        lane = slice(n * BLOCK, (n + 1) * BLOCK)
        dh = nt_dot(scaled, wout[lane, :])
        for q in range(4):
            rows = slice(q * cells, (q + 1) * cells)
            dpb[rows, lane] = (dh * dg[rows, lane]).astype(jnp.bfloat16)
    relay()
    for q in range(4):
        dn = nt_dot(dpb[q * cells : (q + 1) * cells, :], win[...]) * vector(gain)
        parts = [dn[:, c * LANES : (c + 1) * LANES] for c in range(chunks)]
        first = jnp.sum(functools.reduce(jnp.add, parts), axis=1, keepdims=True) / channels
        cross = functools.reduce(jnp.add, [parts[c] * sp[c, q] for c in range(chunks)])
        second = jnp.sum(cross, axis=1, keepdims=True) / channels
        for c in range(chunks):
            back = rstd[q] * (parts[c] - first - sp[c, q] * second)
            back = back.reshape(half, half, LANES)
            for i in range(half):
                gpad[c, reach + 2 * i + q // 2, pl.ds(PAD + q % 2, half, stride=2), :] = back[i]

    tok_moves[0].wait()
    for move in relays:
        move.wait()
    arrived = [(me, tok), (partner, recvt.at[0])]
    for k in range(1, pairs):
        arrived.append((seat(pairs - k, core), recvt.at[k]))
        arrived.append((seat(pairs - k, 1 - core), recvr.at[k - 1]))
    outs = [None] * slots
    for who, block in arrived:
        mine, before = place_of(who)
        for s in range(slots):
            part = block[...] * wide(jnp.logical_and(mine, before == s))
            outs[s] = part if outs[s] is None else outs[s] + part
    for s in range(slots):
        tokout[s] = outs[s]


def tail(taps, gpad, dww, gq, tokout, tok_hbm, dx_hbm, obuf, sems):
    chunks = gpad.shape[0]
    side = dx_hbm.shape[0]
    half = side // 2
    copies = [pltpu.make_async_copy(tokout, tok_hbm, sems.at[chunks])]
    copies[0].start()
    for c in range(chunks):
        outs = depthwise(gpad, dww, c, taps, side, True)
        direct = jnp.broadcast_to(gq[c][:, None], (half, 2, half, LANES)).reshape(side, half, LANES)
        for parity in range(2):
            value = outs[parity] + direct
            for i in range(side):
                obuf[c, i, pl.ds(parity, half, stride=2), :] = value[i]
        copy = pltpu.make_async_copy(
            obuf.at[c], dx_hbm.at[:, :, c * LANES : (c + 1) * LANES], sems.at[c]
        )
        copy.start()
        copies.append(copy)
    for copy in copies:
        copy.wait()


def solution(mesh):
    groups, peers = mesh.shape["group"], mesh.shape["peer"]

    def on_device(
        features, image_of_row, llm_peer, token_grads, dw_weight, dw_bias, ln_gain, ln_bias,
        w_in, b_in, w_out, b_out, layer_scale, comp_weight, comp_bias,
    ):
        side, width, channels = features.shape
        slots = token_grads.shape[0]
        hid = w_in.shape[1]
        taps = math.isqrt(dw_weight.shape[0])
        half = side // 2
        cells = half * half
        chunks = channels // LANES
        assert width == side and llm_peer.shape == (1, 1)
        f32, bf16 = jnp.float32, jnp.bfloat16
        padded = (chunks, side + 2 * (taps // 2), side + 2 * PAD, LANES)
        grid = (half + 2, half + 2 * PAD, channels)
        block = (half, half, channels)
        dma = pltpu.SemaphoreType.DMA
        hbm = pl.BlockSpec(memory_space=pltpu.HBM)
        pairs = peers // 2
        assert peers == 2 * pairs and pairs > 1
        vmem = pl.BlockSpec(memory_space=pltpu.VMEM)
        held = (
            pltpu.VMEM(padded, f32),
            pltpu.VMEM((chunks, taps * taps, LANES), f32),
            pltpu.VMEM((chunks, half, half, LANES), f32),
            pltpu.VMEM((slots,) + block, f32),
        )
        state = pl.pallas_call(
            functools.partial(kernel, groups, peers, taps),
            out_shape=held,
            in_specs=[hbm] * 15,
            out_specs=(vmem,) * 4,
            scratch_shapes=[
                pltpu.VMEM(padded, f32),
                *[pltpu.VMEM((channels,), f32)] * 6,
                pltpu.VMEM((hid,), f32),
                pltpu.VMEM(w_in.shape, bf16),
                pltpu.VMEM(w_out.shape, bf16),
                pltpu.VMEM(comp_weight.shape, bf16),
                pltpu.VMEM((slots,) + block, f32),
                pltpu.VMEM((chunks, 4, cells, LANES), f32),
                pltpu.VMEM((4, cells, LANES), f32),
                pltpu.VMEM((4 * cells, channels), bf16),
                pltpu.VMEM((4 * cells, hid), f32),
                pltpu.VMEM((cells, hid), bf16),
                pltpu.VMEM((4 * cells, hid), bf16),
                pltpu.VMEM((peers, 8, LANES), jnp.int32),
                pltpu.VMEM((pairs,) + block, f32),
                pltpu.VMEM((pairs,) + block, f32),
                pltpu.VMEM((pairs - 1,) + block, f32),
                pltpu.VMEM((pairs - 1,) + block, f32),
                pltpu.VMEM(block, f32),
                pltpu.VMEM((pairs,) + block, f32),
                pltpu.VMEM((pairs - 1,) + block, f32),
                pltpu.VMEM(grid, f32),
                pltpu.VMEM(grid, f32),
                pltpu.VMEM((2, half, channels), f32),
                pltpu.VMEM((2, half, channels), f32),
                pltpu.VMEM((8, half, channels), f32),
                pltpu.VMEM((8, half, channels), f32),
                pltpu.SMEM(image_of_row.shape, jnp.int32),
                pltpu.SMEM((1, 1), jnp.int32),
                dma((2 * chunks + 13,)),
                dma((peers - 1,)),
                dma((peers - 1,)),
                dma,
                dma,
                dma((pairs - 1,)),
                dma((pairs - 1,)),
                dma((pairs,)),
                dma((pairs,)),
                dma((pairs - 1,)),
                dma((pairs - 1,)),
                dma((8,)),
                dma((8,)),
                dma((8,)),
                dma((8,)),
            ],
            compiler_params=pltpu.CompilerParams(collective_id=0, has_side_effects=True),
        )(
            image_of_row,
            llm_peer,
            features,
            token_grads.reshape((slots,) + block),
            dw_weight,
            dw_bias,
            ln_gain,
            ln_bias,
            w_in,
            b_in,
            w_out,
            b_out,
            layer_scale,
            comp_weight,
            comp_bias,
        )
        tokens, grads = pl.pallas_call(
            functools.partial(tail, taps),
            out_shape=(
                jax.ShapeDtypeStruct((slots,) + block, f32),
                jax.ShapeDtypeStruct(features.shape, f32),
            ),
            in_specs=[vmem] * 4,
            out_specs=(hbm, hbm),
            scratch_shapes=[pltpu.VMEM((chunks, side, side, LANES), f32), dma((chunks + 1,))],
            compiler_params=pltpu.CompilerParams(vmem_limit_bytes=16 << 20),
        )(*state)
        return tokens.reshape(slots, cells, channels), grads

    placed = [P()] * 15
    placed[0] = P("group", "peer", None)
    placed[2] = P(("group", "peer"), None)
    placed[3] = P(("group", "peer"), None, None)
    return jax.shard_map(
        on_device,
        mesh=mesh,
        in_specs=tuple(placed),
        out_specs=(P(("group", "peer"), None, None), P("group", "peer", None)),
        check_vma=False,
    )
```
